32 devices in a mesh: trial: 4 (over y, x), rows: 2 (over core), cols: 4 (over z).
Axes of the slice: x: 2, y: 2, z: 4, core: 2. Of those that a mesh axis runs over, the one named last changes fastest.
Arguments:
- weight_gate: float32 [8192, 8192], P(('trial', 'rows'), 'cols'), parts along dimension 0, may hold values from -0.1875 to 0.1875
- moment_gate: float32 [8192, 8192], P(('trial', 'rows'), 'cols'), parts along dimension 0, may hold values from -6 to 6
- square_gate: float32 [8192, 8192], P(('trial', 'rows'), 'cols'), parts along dimension 0, may hold values from 0.1 to 10
- weight_up: float32 [8192, 8192], P(('trial', 'rows'), 'cols'), parts along dimension 0, may hold values from -0.1875 to 0.1875
- moment_up: float32 [8192, 8192], P(('trial', 'rows'), 'cols'), parts along dimension 0, may hold values from -6 to 6
- square_up: float32 [8192, 8192], P(('trial', 'rows'), 'cols'), parts along dimension 0, may hold values from 0.1 to 10
- norm_gain: float32 [8192], P(('trial', 'rows')), parts along dimension 0, may hold values from 0.25 to 1.75
Outputs:
- serving_gate: bfloat16 [8192, 8192], P('trial', 'cols'), parts along dimension 0
- serving_up: bfloat16 [8192, 8192], P('trial', 'cols'), parts along dimension 0
- column_gate: float32 [32768], P(('trial', 'cols')), parts along dimension 0
- column_up: float32 [32768], P(('trial', 'cols')), parts along dimension 0
The draws below stay inside these ranges and needn't reach their ends.
There are 4 independent parts, one for each index of `trial`. The reference program is written for one: setup_inputs(seed, part) draws one part's arguments, and reference() takes and returns one part's arrays. A program takes and returns all parts, laid end to end along the dimension named above; each array names one. Nothing has to cross between parts.
All inputs are finite; a program needn't handle non-finite values. Where the reference program divides by a largest or mean magnitude, that divisor is 1e-20 or more.
Results may differ from the reference program's by a relative error of at most 0.001.
Values may be sent and summed in bfloat16 or wider, within the bound.
No kernel may reach another device: no remote copies, remote signals or barrier semaphores. Data moves between devices by JAX's collectives and lax.ppermute only.
A program may use at most 128 MiB of HBM per device.

```python
import math
import jax
import jax.numpy as jnp
from jax import lax

D_MODEL = 2048
D_INNER = 8192


def strengthened(array, stream_key, source, target, blocks, factor):
    def block_of(dim):
        return (jnp.arange(array.shape[dim]) // (array.shape[dim] // blocks)).reshape((-1,) + (1,) * (array.ndim - 1 - dim))

    first = jax.random.permutation(stream_key, blocks)[block_of(target)]
    far = (block_of(target) + blocks // 2) % blocks
    return jnp.where((block_of(source) == first) | (block_of(source) == far), factor * array, array)


def shard_levels(stream_key, extent, cuts, least, high):
    def one(axis_at, shards_of):
        draws = jax.random.uniform(jax.random.fold_in(jax.random.fold_in(stream_key, 6), axis_at), (shards_of,), jnp.float32, least / len(cuts), high / len(cuts))
        return jnp.repeat(jnp.exp(draws), extent[axis_at] // shards_of).reshape((-1,) + (1,) * (len(extent) - axis_at - 1))

    level = one(*cuts[0])
    for cut in cuts[1:]:
        level = level * one(*cut)
    return level


def gaussian(own_key, extent, width, bound, split=(), held_as=jnp.bfloat16):
    drawn = jax.random.normal(own_key, extent, jnp.float32) * width
    if len(split) > 0:
        drawn = shard_levels(own_key, extent, split, -0.22, 0.18) * drawn
    return jnp.clip(drawn, min=-bound, max=bound).astype(held_as)


def bell_draw_with(key, extent, width, bound, shards, heavy, kind=jnp.bfloat16):
    values = width * jax.random.normal(key, extent, jnp.float32)
    if shards:
        values = values * shard_levels(key, extent, shards, -0.22, 0.18)
    return jnp.clip(strengthened(values, jax.random.fold_in(key, 3), *heavy), -bound, bound).astype(kind)


def setup_inputs(seed: int = 0, part: int = 0) -> dict:
    splits = jax.random.split(jax.random.key(seed), 8)
    own_keys = jax.random.split(jax.random.fold_in(splits[7], part), 8)
    return {
        "weight_gate": bell_draw_with(own_keys[0], (D_MODEL, D_INNER), D_MODEL ** -0.5, 0.1875, ((0, 2), (1, 4)), (0, 1, 4, 2.0), jnp.float32),
        "moment_gate": gaussian(own_keys[1], (D_MODEL, D_INNER), 1.0, 6.0, ((0, 2), (1, 4)), jnp.float32),
        "square_gate": jnp.clip(jnp.exp(math.log(10.0) - 4.6051702 * jax.random.uniform(own_keys[2], (D_MODEL, D_INNER), jnp.float32) ** shard_levels(own_keys[2], (D_MODEL, D_INNER), ((0, 2), (1, 4)), -0.2, 0.2)), 0.1, 10.0),
        "weight_up": bell_draw_with(own_keys[3], (D_MODEL, D_INNER), D_MODEL ** -0.5, 0.1875, ((0, 2), (1, 4)), (0, 1, 4, 2.0), jnp.float32),
        "moment_up": gaussian(own_keys[4], (D_MODEL, D_INNER), 1.0, 6.0, ((0, 2), (1, 4)), jnp.float32),
        "square_up": jnp.clip(jnp.exp(math.log(10.0) - 4.6051702 * jax.random.uniform(own_keys[5], (D_MODEL, D_INNER), jnp.float32) ** shard_levels(own_keys[5], (D_MODEL, D_INNER), ((0, 2), (1, 4)), -0.2, 0.2)), 0.1, 10.0),
        "norm_gain": jnp.clip(1.0 + 0.15 * jax.random.normal(own_keys[6], (D_MODEL,), jnp.float32), 0.25, 1.75),
    }


learn_rate = 0.02
decay_rate = 0.05
tiny_value = 1e-08

def reference(weight_gate, moment_gate, square_gate, weight_up, moment_up, square_up, norm_gain):
    whole_gate = weight_gate - learn_rate * (moment_gate / (jnp.sqrt(square_gate) + tiny_value) + decay_rate * weight_gate)
    whole_up = weight_up - learn_rate * (moment_up / (jnp.sqrt(square_up) + tiny_value) + decay_rate * weight_up)
    whole_gained_gate = whole_gate * norm_gain[:, None]
    whole_gained_up = whole_up * norm_gain[:, None]
    column_gate = lax.optimization_barrier(jnp.sum(jnp.abs(whole_gained_gate), axis=0)) / D_MODEL
    serving_gate = (whole_gained_gate / column_gate).astype(jnp.bfloat16)
    column_up = lax.optimization_barrier(jnp.sum(jnp.abs(whole_gained_up), axis=0)) / D_MODEL
    serving_up = (whole_gained_up / column_up).astype(jnp.bfloat16)
    return (serving_gate, serving_up, column_gate, column_up)
```

```python
import functools

import jax
import jax.numpy as jnp
from jax import lax
from jax.experimental import pallas as pl
from jax.experimental.pallas import tpu as pltpu
from jax.sharding import PartitionSpec as P

learn_rate = 0.02
decay_rate = 0.05
tiny_value = 1e-08
keep_rate = 1.0 - learn_rate * decay_rate

UNITS = 2
FOLD = 2
LANES = 128


def update_kernel(
    after_ref, gain_ref, weight_ref, moment_ref, square_ref, gained_ref, sums_ref, part_ref, spread_ref, *, block, fold
):
    step = pl.program_id(0)
    width = weight_ref.shape[1]

    def spread(at, slot):
        for n in range(fold):
            line = gain_ref[pl.ds(at * fold + n, 1), :]
            spread_ref[slot, n * block : (n + 1) * block, :] = jnp.broadcast_to(line, (LANES, block)).T

    @pl.when(step == 0)
    def _():
        part_ref[...] = jnp.zeros_like(part_ref)
        spread(0, 0)

    spread(jnp.minimum(step + 1, pl.num_programs(0) - 1), (step + 1) % 2)
    for n in range(fold):
        inner = slice(n * block, (n + 1) * block)
        rows = pl.ds(pl.multiple_of((step * fold + n) * block, block), block)
        gain = spread_ref[step % 2, inner, :]
        keep = keep_rate * gain
        move = learn_rate * gain
        for at in range(0, width, LANES):
            lanes = slice(at, at + LANES)
            square = square_ref[inner, lanes]
            divisor = square * lax.rsqrt(square) + tiny_value
            direction = moment_ref[inner, lanes] * lax.rsqrt(divisor * divisor)
            gained = keep * weight_ref[inner, lanes] - move * direction
            gained_ref[rows, lanes] = gained
            part_ref[:, lanes] += jnp.sum(jnp.abs(gained).reshape(block // 8, 8, LANES), axis=0)

    @pl.when(step == pl.num_programs(0) - 1)
    def _():
        sums_ref[...] = jnp.sum(part_ref[...], axis=0, keepdims=True)


def update(after, gain, weight, moment, square, chunk, width):
    rows = weight.shape[0]
    block = min(rows, LANES)
    fold = FOLD if rows % (block * FOLD) == 0 else 1
    spec = pl.BlockSpec((block * fold, width), lambda i: (i, chunk))
    whole = pl.BlockSpec(memory_space=pltpu.VMEM)
    elements = rows * width
    return pl.pallas_call(
        functools.partial(update_kernel, block=block, fold=fold),
        grid=(rows // block // fold,),
        in_specs=[pl.BlockSpec(memory_space=pl.ANY), whole, spec, spec, spec],
        out_specs=[whole, whole],
        out_shape=[pltpu.VMEM((rows, width), jnp.float32), pltpu.VMEM((1, width), jnp.float32)],
        scratch_shapes=[pltpu.VMEM((8, width), jnp.float32), pltpu.VMEM((2, fold * block, LANES), jnp.float32)],
        compiler_params=pltpu.CompilerParams(vmem_limit_bytes=24 << 20),
        cost_estimate=pl.CostEstimate(flops=elements * 1000, bytes_accessed=elements * 12, transcendentals=elements * 2),
        name="update",
    )(after, *(pltpu.with_memory_space_constraint(array, pltpu.HBM) for array in (gain, weight, moment, square)))


def scale_kernel(*refs, total_rows):
    gained_ref, *sum_refs, narrow_ref, column_ref = refs
    total = sum_refs[0][...]
    for ref in sum_refs[1:]:
        total = total + ref[...]
    column = total / total_rows
    column_ref[...] = column
    inverse = 1.0 / column
    rows, width = gained_ref.shape
    block = min(rows, 64)
    factors = [jnp.broadcast_to(inverse[:, at : at + LANES], (8, LANES)) for at in range(0, width, LANES)]

    def body(i, _):
        here = pl.ds(pl.multiple_of(i * block, block), block)
        for n, factor in enumerate(factors):
            lanes = slice(n * LANES, (n + 1) * LANES)
            values = gained_ref[here, lanes].reshape(block // 8, 8, LANES) * factor
            narrow_ref[here, lanes] = values.reshape(block, LANES).astype(jnp.bfloat16)
        return 0

    lax.fori_loop(0, rows // block, body, 0)


def scale(gained, sums, total_rows):
    rows, width = gained.shape
    whole = pl.BlockSpec(memory_space=pltpu.VMEM)
    elements = rows * width
    return pl.pallas_call(
        functools.partial(scale_kernel, total_rows=total_rows),
        in_specs=[whole] * (1 + len(sums)),
        out_specs=[whole, whole],
        out_shape=[pltpu.VMEM((rows, width), jnp.bfloat16), pltpu.VMEM((1, width), jnp.float32)],
        compiler_params=pltpu.CompilerParams(vmem_limit_bytes=4 << 20),
        cost_estimate=pl.CostEstimate(flops=elements * 200, bytes_accessed=elements, transcendentals=0),
        name="scale",
    )(pltpu.with_memory_space_constraint(gained, pltpu.VMEM), *sums)


def place_kernel(*refs, row_devices, count, n_outs, n_held, where, width):
    parts = refs[:count]
    outs = refs[count + n_held : count + n_held + n_outs]
    me = lax.axis_index("rows")
    sems = refs[-1]
    copies = []
    for n, (out, hop, chunk) in enumerate(where):
        rows = parts[n].shape[0]
        target = outs[out].at[pl.ds(pl.multiple_of(lax.rem(me + (row_devices - hop), row_devices) * rows, rows), rows), pl.ds(chunk * width, width)]
        copies.append(pltpu.make_async_copy(parts[n], target, sems.at[n]))
    for copy in copies:
        copy.start()
    for copy in copies:
        copy.wait()


def place(row_devices, parts, where, held, out_shapes):
    width = parts[0].shape[1]
    n_held = len(held)
    elements = sum(part.size for part in parts)
    return pl.pallas_call(
        functools.partial(
            place_kernel, row_devices=row_devices, count=len(parts), n_outs=len(out_shapes), n_held=n_held, where=tuple(where), width=width
        ),
        in_specs=[pl.BlockSpec(memory_space=pl.ANY)] * (len(parts) + n_held),
        out_specs=[pl.BlockSpec(memory_space=pl.ANY)] * len(out_shapes),
        out_shape=out_shapes,
        input_output_aliases={len(parts) + n: n for n in range(n_held)},
        scratch_shapes=[pltpu.SemaphoreType.DMA((len(parts),))],
        compiler_params=pltpu.CompilerParams(vmem_limit_bytes=1 << 20),
        cost_estimate=pl.CostEstimate(flops=elements * 400, bytes_accessed=elements * 4, transcendentals=0),
        name="place",
    )(*(pltpu.with_memory_space_constraint(part, pltpu.VMEM) for part in parts), *held)


def shards(row_devices, weight_gate, moment_gate, square_gate, weight_up, moment_up, square_up, norm_gain):
    rows, columns = weight_gate.shape
    chunks = UNITS // 2
    width = columns // chunks
    sources = ((weight_gate, moment_gate, square_gate), (weight_up, moment_up, square_up))
    units = [(which, chunk) for which in range(2) for chunk in range(chunks)]
    gain = norm_gain.reshape(-1, min(rows, LANES))

    def rotations(value):
        return [
            lax.ppermute(value, "rows", [(j, (j + hop) % row_devices) for j in range(row_devices)])
            for hop in range(1, row_devices)
        ]

    pieces, scales = [], []
    pending = None
    ready = gain

    def finish(unit, gained, all_sums):
        narrow, column = scale(gained, all_sums, rows * row_devices)
        pieces.append((unit, [narrow] + rotations(narrow)))
        scales.append(column)
        return narrow

    history = []
    for unit in units:
        which, chunk = unit
        if len(history) >= 2:
            ready = finish(*history[len(history) - 2])
        gained, sums = update(ready, gain, *sources[which], chunk, width)
        history.append((unit, gained, [sums] + rotations(sums)))
    for entry in history[max(len(history) - 2, 0):]:
        finish(*entry)

    first, last = [], []
    for n, ((which, chunk), held) in enumerate(pieces):
        for hop, part in enumerate(held):
            group = last if hop > 0 and n == len(pieces) - 1 else first
            group.append((part, (which, hop, chunk)))
    out = jax.ShapeDtypeStruct((rows * row_devices, columns), jnp.bfloat16)
    outs = place(row_devices, [p for p, _ in first], [w for _, w in first], (), [out, out])
    if last:
        outs = [outs[0], *place(row_devices, [p for p, _ in last], [(0, h, c) for _, (_, h, c) in last], (outs[1],), [out])]
    column_gate = jnp.concatenate([c.reshape(-1) for c in scales[:chunks]])
    column_up = jnp.concatenate([c.reshape(-1) for c in scales[chunks:]])
    return (outs[0], outs[1], column_gate, column_up)


def solution(mesh):
    matrix = P(("trial", "rows"), "cols")
    return jax.shard_map(
        functools.partial(shards, mesh.shape["rows"]),
        mesh=mesh,
        in_specs=(matrix,) * 6 + (P(("trial", "rows")),),
        out_specs=(P("trial", "cols"), P("trial", "cols"), P(("trial", "cols")), P(("trial", "cols"))),
        check_vma=False,
    )
```

```python
import functools

import jax
import jax.numpy as jnp
from jax import lax
from jax.experimental import pallas as pl
from jax.experimental.pallas import tpu as pltpu
from jax.sharding import PartitionSpec as P

learn_rate = 0.02
decay_rate = 0.05
tiny_value = 1e-08
keep_rate = 1.0 - learn_rate * decay_rate

UNITS = 2
BLOCK = 64
AHEAD = 8
LANES = 128


def update_kernel(
    after_ref, gain_ref, weight_ref, moment_ref, square_ref, gained_ref, sums_ref,
    gains, moments, squares, part_ref, keep_ref, move_ref, sems, gain_sem, *, block, chunk, held
):
    rows, width = gained_ref.shape
    count = rows // block
    columns = pl.ds(chunk * width, width)

    weights = weight_ref if held else gained_ref
    def copies(at):
        here = pl.ds(pl.multiple_of(at * block, block), block)
        return [
            pltpu.make_async_copy(source.at[here, columns], target.at[here, :], sems.at[n, at])
            for n, (source, target) in enumerate(
                ((square_ref, squares), (moment_ref, moments), (weight_ref, gained_ref))[: 2 if held else 3]
            )
        ]

    def start(at):
        for copy in copies(at):
            copy.start()

    fetch = pltpu.make_async_copy(gain_ref, gains, gain_sem)
    fetch.start()
    ahead = min(AHEAD, count)
    for at in range(ahead):
        start(at)

    fetch.wait()
    run = gains.shape[1]
    for n in range(gains.shape[0]):
        gain = jnp.broadcast_to(gains[n : n + 1, :], (LANES, run)).T
        keep_ref[n * run : (n + 1) * run, :] = keep_rate * gain
        move_ref[n * run : (n + 1) * run, :] = learn_rate * gain
    part_ref[...] = jnp.zeros_like(part_ref)

    def body(at, _):
        @pl.when(at + ahead < count)
        def _():
            start(at + ahead)

        for copy in copies(at):
            copy.wait()
        lanes = [slice(n, n + LANES) for n in range(0, width, LANES)]
        part = [part_ref[:, tile] for tile in lanes]
        for row in range(0, block, 8):
            here = pl.ds(pl.multiple_of(at * block + row, 8), 8)
            keep = keep_ref[here, :]
            move = move_ref[here, :]
            for n, tile in enumerate(lanes):
                square = squares[here, tile]
                divisor = square * lax.rsqrt(square) + tiny_value
                direction = moments[here, tile] * lax.rsqrt(divisor * divisor)
                gained = keep * weights[here, tile] - move * direction
                gained_ref[here, tile] = gained
                part[n] = part[n] + jnp.abs(gained)
        for n, tile in enumerate(lanes):
            part_ref[:, tile] = part[n]
        return 0

    lax.fori_loop(0, count, body, 0)
    sums_ref[...] = jnp.sum(part_ref[...], axis=0, keepdims=True)


def update(after, gain, weight, moment, square, chunk, width, held):
    rows = weight.shape[0]
    block = BLOCK if rows % BLOCK == 0 else rows
    whole = pl.BlockSpec(memory_space=pltpu.VMEM)
    far = pl.BlockSpec(memory_space=pl.ANY)
    elements = rows * width
    return pl.pallas_call(
        functools.partial(update_kernel, block=block, chunk=chunk, held=held),
        in_specs=[far, far, whole if held else far, far, far],
        out_specs=[whole, whole],
        out_shape=[pltpu.VMEM((rows, width), jnp.float32), pltpu.VMEM((1, width), jnp.float32)],
        scratch_shapes=[
            pltpu.VMEM(gain.shape, jnp.float32),
            pltpu.VMEM((rows, width), jnp.float32),
            pltpu.VMEM((rows, width), jnp.float32),
            pltpu.VMEM((8, width), jnp.float32),
            pltpu.VMEM((rows, LANES), jnp.float32),
            pltpu.VMEM((rows, LANES), jnp.float32),
            pltpu.SemaphoreType.DMA((3, rows // block)),
            pltpu.SemaphoreType.DMA,
        ],
        compiler_params=pltpu.CompilerParams(vmem_limit_bytes=elements * 8 + (3 << 20)),
        cost_estimate=pl.CostEstimate(flops=elements * 1000, bytes_accessed=elements * 12, transcendentals=elements * 2),
        name="update",
    )(
        after,
        *(
            pltpu.with_memory_space_constraint(array, pltpu.VMEM if held and n == 1 else pltpu.HBM)
            for n, array in enumerate((gain, weight, moment, square))
        ),
    )


def scale_kernel(*refs, total_rows):
    gained_ref, *sum_refs, narrow_ref, column_ref = refs
    total = sum_refs[0][...]
    for ref in sum_refs[1:]:
        total = total + ref[...]
    column = total / total_rows
    column_ref[...] = column
    inverse = 1.0 / column
    rows, width = gained_ref.shape
    block = min(rows, 64)
    factors = [jnp.broadcast_to(inverse[:, at : at + LANES], (8, LANES)) for at in range(0, width, LANES)]

    def body(i, _):
        here = pl.ds(pl.multiple_of(i * block, block), block)
        for n, factor in enumerate(factors):
            lanes = slice(n * LANES, (n + 1) * LANES)
            values = gained_ref[here, lanes].reshape(block // 8, 8, LANES) * factor
            narrow_ref[here, lanes] = values.reshape(block, LANES).astype(jnp.bfloat16)
        return 0

    lax.fori_loop(0, rows // block, body, 0)


def scale(gained, sums, total_rows):
    rows, width = gained.shape
    whole = pl.BlockSpec(memory_space=pltpu.VMEM)
    elements = rows * width
    return pl.pallas_call(
        functools.partial(scale_kernel, total_rows=total_rows),
        in_specs=[whole] * (1 + len(sums)),
        out_specs=[whole, whole],
        out_shape=[pltpu.VMEM((rows, width), jnp.bfloat16), pltpu.VMEM((1, width), jnp.float32)],
        compiler_params=pltpu.CompilerParams(vmem_limit_bytes=4 << 20),
        cost_estimate=pl.CostEstimate(flops=elements * 200, bytes_accessed=elements, transcendentals=0),
        name="scale",
    )(pltpu.with_memory_space_constraint(gained, pltpu.VMEM), *sums)


def place_kernel(*refs, row_devices, count, n_outs, n_held, where, width):
    parts = refs[:count]
    outs = refs[count + n_held : count + n_held + n_outs]
    me = lax.axis_index("rows")
    sems = refs[-1]
    copies = []
    for n, (out, hop, chunk) in enumerate(where):
        rows = parts[n].shape[0]
        target = outs[out].at[pl.ds(pl.multiple_of(lax.rem(me + (row_devices - hop), row_devices) * rows, rows), rows), pl.ds(chunk * width, width)]
        copies.append(pltpu.make_async_copy(parts[n], target, sems.at[n]))
    for copy in copies:
        copy.start()
    for copy in copies:
        copy.wait()


def place(row_devices, parts, where, held, out_shapes):
    width = parts[0].shape[1]
    n_held = len(held)
    elements = sum(part.size for part in parts)
    return pl.pallas_call(
        functools.partial(
            place_kernel, row_devices=row_devices, count=len(parts), n_outs=len(out_shapes), n_held=n_held, where=tuple(where), width=width
        ),
        in_specs=[pl.BlockSpec(memory_space=pl.ANY)] * (len(parts) + n_held),
        out_specs=[pl.BlockSpec(memory_space=pl.ANY)] * len(out_shapes),
        out_shape=out_shapes,
        input_output_aliases={len(parts) + n: n for n in range(n_held)},
        scratch_shapes=[pltpu.SemaphoreType.DMA((len(parts),))],
        compiler_params=pltpu.CompilerParams(vmem_limit_bytes=1 << 20),
        cost_estimate=pl.CostEstimate(flops=elements * 400, bytes_accessed=elements * 4, transcendentals=0),
        name="place",
    )(*(pltpu.with_memory_space_constraint(part, pltpu.VMEM) for part in parts), *held)


def shards(row_devices, weight_gate, moment_gate, square_gate, weight_up, moment_up, square_up, norm_gain):
    rows, columns = weight_gate.shape
    chunks = UNITS // 2
    width = columns // chunks
    sources = ((weight_gate, moment_gate, square_gate), (weight_up, moment_up, square_up))
    units = [(which, chunk) for which in range(2) for chunk in range(chunks)]
    gain = norm_gain.reshape(-1, min(rows, LANES))

    def rotations(value):
        return [
            lax.ppermute(value, "rows", [(j, (j + hop) % row_devices) for j in range(row_devices)])
            for hop in range(1, row_devices)
        ]

    pieces, scales = [], []
    pending = None
    ready = gain

    def finish(unit, gained, all_sums):
        narrow, column = scale(gained, all_sums, rows * row_devices)
        pieces.append((unit, [narrow] + rotations(narrow)))
        scales.append(column)
        return narrow

    history = []
    for unit in units:
        which, chunk = unit
        if len(history) >= 2:
            ready = finish(*history[len(history) - 2])
        gained, sums = update(ready, gain, *sources[which], chunk, width, chunks == 1 and which == 1)
        history.append((unit, gained, [sums] + rotations(sums)))
    for entry in history[max(len(history) - 2, 0):]:
        finish(*entry)

    first, last = [], []
    for n, ((which, chunk), held) in enumerate(pieces):
        for hop, part in enumerate(held):
            group = last if hop > 0 and n == len(pieces) - 1 else first
            group.append((part, (which, hop, chunk)))
    out = jax.ShapeDtypeStruct((rows * row_devices, columns), jnp.bfloat16)
    outs = place(row_devices, [p for p, _ in first], [w for _, w in first], (), [out, out])
    if last:
        outs = [outs[0], *place(row_devices, [p for p, _ in last], [(0, h, c) for _, (_, h, c) in last], (outs[1],), [out])]
    column_gate = jnp.concatenate([c.reshape(-1) for c in scales[:chunks]])
    column_up = jnp.concatenate([c.reshape(-1) for c in scales[chunks:]])
    return (outs[0], outs[1], column_gate, column_up)


def solution(mesh):
    matrix = P(("trial", "rows"), "cols")
    return jax.shard_map(
        functools.partial(shards, mesh.shape["rows"]),
        mesh=mesh,
        in_specs=(matrix,) * 6 + (P(("trial", "rows")),),
        out_specs=(P("trial", "cols"), P("trial", "cols"), P(("trial", "cols")), P(("trial", "cols"))),
        check_vma=False,
    )
```
